32 devices in a mesh: groups: 2 (over y), expert: 4 (over z), mp: 4 (over x, core).
Axes of the slice: x: 2, y: 2, z: 4, core: 2. Of those that a mesh axis runs over, the one named last changes fastest.
Arguments:
- tokens: bfloat16 [6144, 1024], P(('groups', 'expert'), 'mp'), parts along dimension 0, may hold values from -60 to 60
- gain: float32 [1024], replicated, may hold values from 0.1 to 1.9
- w_res_in: bfloat16 [1024, 4096], P(None, 'mp'), may hold values from -0.1875 to 0.1875
- w_res_out: bfloat16 [4096, 1024], P('mp'), may hold values from -0.09375 to 0.09375
- w_exp_in: bfloat16 [4, 1024, 4096], P('expert', None, 'mp'), may hold values from -0.1875 to 0.1875
- w_exp_out: bfloat16 [4, 4096, 1024], P('expert', 'mp'), may hold values from -0.09375 to 0.09375
- expert_of: int32 [6144], P(('groups', 'expert')), parts along dimension 0, may hold values from 0 to 3
- slot_of: int32 [6144], P(('groups', 'expert')), parts along dimension 0, may hold values from -1 to 239, as said below
- gate_prob: float32 [6144], P(('groups', 'expert')), parts along dimension 0, may hold values from 0.2 to 1
Outputs:
- layer_out: bfloat16 [6144, 1024], P(('groups', 'expert'), 'mp'), parts along dimension 0
The draws below stay inside these ranges and needn't reach their ends.
There are 2 independent parts, one for each index of `groups`. The reference program is written for one: setup_inputs(seed, part) draws one part's arguments, and reference() takes and returns one part's arrays. A program takes and returns all parts, laid end to end along the dimension named above; an argument that names none is the same for every part. Nothing has to cross between parts.
Inputs may be any that keep to these rules, and one draw needn't show every extreme that they name: slot_of[t] is the number of earlier tokens of t's aligned block of 768 tokens with the same expert_of, or -1 where that number is 240 or more. In every draw one expert has more than 240 tokens in every aligned block.
All inputs are finite; a program needn't handle non-finite values.
Results may differ from the reference program's by a relative error of at most 0.014.
Values may be sent and summed in bfloat16 or wider, within the bound.
A program may use at most 64 MiB of HBM per device.

```python
import math
import jax
import jax.numpy as jnp
from jax import lax

D = 1024
FE = 4096
FR = 4096
TOK_DEV = 768
EXPERTS = 4
TOKENS = 3072
CAP = 240
N_EXPERT = 4
N_MP = 4


def draw_tokens(key, part):
    mixed = jax.random.fold_in(key, 11)
    key_base, key_rows, key_cols = jax.random.split(mixed, 3)
    base = jnp.clip(jax.random.normal(key_base, (TOKENS, D), jnp.float32), -5.5, 5.5)
    row_scale = jnp.exp(jax.random.uniform(key_rows, (TOKENS, 1), jnp.float32) * math.log(10.0))
    col_scale = jnp.exp(jax.random.uniform(key_cols, (1, D), jnp.float32) * math.log(10.0))
    return (base * row_scale * col_scale / 10.0).astype(jnp.bfloat16)


def shuffle(subkey):
    return jax.random.permutation(subkey, TOK_DEV)


def routing_pair(key):
    mixed = jax.random.fold_in(key, 5)
    key_base, key_hot, key_perm = jax.random.split(mixed, 3)
    blocks = TOKENS // TOK_DEV
    base = jax.random.randint(key_base, (blocks, TOK_DEV), 0, EXPERTS)
    hottest = jax.random.randint(key_hot, (1, 1), 0, EXPERTS)
    order = jax.vmap(shuffle)(jax.random.split(key_perm, blocks))
    chosen = order < CAP + 2
    expert_ids = jnp.where(chosen, hottest, base).astype(jnp.int32)
    same = expert_ids[:, :, None] == expert_ids[:, None, :]
    index = jnp.arange(TOK_DEV, dtype=jnp.int32)
    earlier = index[None, :] < index[:, None]
    rank = jnp.sum(jnp.logical_and(same, earlier[None]).astype(jnp.int32), axis=2)
    slots = jnp.where(rank < CAP, rank, -1).astype(jnp.int32)
    return (expert_ids.reshape(TOKENS), slots.reshape(TOKENS))


def draw_expert_of(key, part):
    return routing_pair(key)[0]


def draw_slot_of(key, part):
    return routing_pair(key)[1]


def level_of(own_key, extent, shards, low, largest):
    loudness = 1.0
    for axis_at, parts in shards:
        heights = jax.random.uniform(jax.random.fold_in(jax.random.fold_in(own_key, 6), axis_at), (parts,), jnp.float32, low / len(shards), largest / len(shards))
        loudness = loudness * jnp.repeat(jnp.exp(heights), extent[axis_at] // parts).reshape((-1,) + (1,) * (len(extent) - 1 - axis_at))
    return loudness


def gaussian(stream_key, dims, deviation, most, shards=(), kind=jnp.bfloat16):
    result = jax.random.normal(stream_key, dims, jnp.float32) * deviation
    if len(shards) > 0:
        result = level_of(stream_key, dims, shards, -0.22, 0.18) * result
    return jnp.clip(result, min=-most, max=most).astype(kind)


def setup_inputs(seed: int = 0, part: int = 0) -> dict:
    arg_keys = jax.random.split(jax.random.key(seed), 10)
    part_keys = jax.random.split(jax.random.fold_in(arg_keys[9], part), 10)
    return {
        "tokens": draw_tokens(jax.random.fold_in(jax.random.fold_in(arg_keys[9], part), 71), part),
        "gain": jnp.clip(1.0 + 0.18 * jax.random.normal(arg_keys[1], (D,), jnp.float32), 0.1, 1.9),
        "w_res_in": gaussian(arg_keys[2], (D, FR), D ** -0.5, 0.1875, ((1, 4),)),
        "w_res_out": gaussian(arg_keys[3], (FR, D), FR ** -0.5, 0.09375, ((0, 4),)),
        "w_exp_in": gaussian(arg_keys[4], (EXPERTS, D, FE), D ** -0.5, 0.1875, ((0, 4), (2, 4))),
        "w_exp_out": gaussian(arg_keys[5], (EXPERTS, FE, D), FE ** -0.5, 0.09375, ((0, 4), (1, 4))),
        "expert_of": draw_expert_of(jax.random.fold_in(jax.random.fold_in(arg_keys[9], part), 71), part),
        "slot_of": draw_slot_of(jax.random.fold_in(jax.random.fold_in(arg_keys[9], part), 71), part),
        "gate_prob": jnp.clip(jnp.exp(math.log(1.0) - 1.609438 * jax.random.uniform(part_keys[8], (TOKENS,), jnp.float32) ** level_of(part_keys[8], (TOKENS,), ((0, 4),), -0.2, 0.2)), 0.2, 1.0),
    }


def rms_rows(tokens, gain):
    values = tokens.astype(jnp.float32)
    inverse = lax.rsqrt(lax.optimization_barrier(jnp.mean(values * values, axis=-1, keepdims=True)) + 1e-05)
    return (values * inverse * gain.astype(jnp.float32)).astype(jnp.bfloat16)

def block_sums(hidden, w_out):
    width = hidden.shape[1] // N_MP
    total = jnp.zeros((hidden.shape[0], w_out.shape[1]), jnp.float32)
    for block in range(N_MP):
        part = jnp.dot(hidden[:, block * width:(block + 1) * width], w_out[block * width:(block + 1) * width], preferred_element_type=jnp.float32)
        total = total + part.astype(jnp.bfloat16).astype(jnp.float32)
    return total

def reference(tokens, gain, w_res_in, w_res_out, w_exp_in, w_exp_out, expert_of, slot_of, gate_prob):
    normed = rms_rows(tokens, gain)
    res_hidden = jax.nn.gelu(jnp.dot(normed, w_res_in, preferred_element_type=jnp.float32)).astype(jnp.bfloat16)
    res_sum = block_sums(res_hidden, w_res_out)
    blocks = N_EXPERT
    position = jnp.arange(TOKENS, dtype=jnp.int32)
    block_of = position // TOK_DEV
    slots_all = EXPERTS * blocks * CAP
    destination = jnp.where(slot_of >= 0, expert_of * (blocks * CAP) + block_of * CAP + slot_of, slots_all).astype(jnp.int32)
    buffer = jnp.zeros((slots_all + 1, D), jnp.bfloat16).at[destination].set(normed)
    expert_in = buffer[:slots_all].reshape(EXPERTS, blocks * CAP, D)

    def one_expert(item):
        rows, w_in, w_out = item
        hidden = jax.nn.gelu(jnp.dot(rows, w_in, preferred_element_type=jnp.float32)).astype(jnp.bfloat16)
        return block_sums(hidden, w_out).astype(jnp.bfloat16)
    expert_out = lax.map(one_expert, (expert_in, w_exp_in, w_exp_out))
    flat_rows = jnp.concatenate([expert_out.reshape(slots_all, D), jnp.zeros((1, D), jnp.bfloat16)], axis=0)
    moe_value = flat_rows[destination].astype(jnp.float32)
    return (res_sum + gate_prob[:, None] * moe_value).astype(jnp.bfloat16)
```

```python
import jax
import jax.numpy as jnp
from jax import lax
from jax.experimental import pallas as pl
from jax.experimental.pallas import tpu as pltpu
from jax.sharding import PartitionSpec as P


def rms_rows(tokens, gain):
    values = tokens.astype(jnp.float32)
    inverse = lax.rsqrt(jnp.mean(values * values, axis=-1, keepdims=True) + 1e-05)
    return (values * inverse * gain).astype(jnp.bfloat16)


def per_device(
    tokens, gain, w_res_in, w_res_out, w_exp_in, w_exp_out, expert_of, slot_of, gate_prob
):
    full_rows = lax.all_gather(tokens, "mp", axis=1, tiled=True)
    normed = rms_rows(full_rows, gain)
    res_hidden = jax.nn.gelu(jnp.dot(normed, w_res_in, preferred_element_type=jnp.float32)).astype(
        jnp.bfloat16
    )
    res_part = jnp.dot(res_hidden, w_res_out, preferred_element_type=jnp.float32)
    row_count = expert_of.shape[0]
    experts = lax.axis_size("expert")
    capacity = max(2, 5 * row_count // (4 * experts))
    feat_width = tokens.shape[1]
    slot_id = jnp.where(slot_of >= 0, expert_of * capacity + slot_of, -1)
    slot_index = jnp.arange(experts * capacity, dtype=jnp.int32)
    send_table = (slot_index[:, None] == slot_id[None, :]).astype(jnp.bfloat16)
    take_table = (slot_id[:, None] == slot_index[None, :]).astype(jnp.bfloat16)
    local_in = w_exp_in[0]
    local_out = w_exp_out[0]
    mp_index = lax.axis_index("mp")
    own_slice = lax.dynamic_slice_in_dim(normed, mp_index * feat_width, feat_width, 1)
    outgoing = jnp.dot(send_table, own_slice, preferred_element_type=jnp.float32).astype(
        jnp.bfloat16
    )
    incoming = lax.all_to_all(
        outgoing.reshape(experts, capacity, feat_width),
        "expert",
        split_axis=0,
        concat_axis=0,
        tiled=True,
    )
    piece = lax.all_gather(incoming, "mp", axis=2, tiled=True)
    flat_piece = piece.reshape(-1, piece.shape[2])
    preact = jnp.dot(flat_piece, local_in, preferred_element_type=jnp.float32)
    exp_hidden = jax.nn.gelu(preact).astype(jnp.bfloat16)
    exp_part = jnp.dot(exp_hidden, local_out, preferred_element_type=jnp.float32)
    gate_column = gate_prob[:, None]
    summed = lax.psum_scatter(exp_part.astype(jnp.bfloat16), "mp", scatter_dimension=1, tiled=True)
    returned = lax.all_to_all(
        summed.reshape(experts, capacity, feat_width),
        "expert",
        split_axis=0,
        concat_axis=0,
        tiled=True,
    )
    moe_value = jnp.dot(
        take_table,
        returned.reshape(experts * capacity, feat_width),
        preferred_element_type=jnp.float32,
    )
    res_sum = lax.psum_scatter(
        res_part.astype(jnp.bfloat16), "mp", scatter_dimension=1, tiled=True
    ).astype(jnp.float32)
    return (res_sum + gate_column * moe_value).astype(jnp.bfloat16)


MESH = pl.DeviceIdType.MESH
F32 = jnp.float32
BF16 = jnp.bfloat16


def dot(a, b):
    return jnp.dot(a, b, preferred_element_type=F32)


def first_layer(rows_ref, w_ref, hidden_ref, chunk):
    def body(n, carry):
        cols = pl.ds(pl.multiple_of(n * chunk, chunk), chunk)
        hidden_ref[:, cols] = jax.nn.gelu(dot(rows_ref[...], w_ref[:, cols])).astype(BF16)
        return carry

    lax.fori_loop(0, hidden_ref.shape[1] // chunk, body, 0)


def fused_kernel(
    tokens, gain, w_ri_h, w_ro_h, w_ei_h, w_eo_h, expert_of, slot_of, gate_prob, out,
    w_ri, w_ro, w_ei, w_eo, tok, normed, res_hid, rows_raw, out_rows, out_rows2, rows_near, rows_far,
    hid, own_part, de_send, de_recv, e_keep, pair_send, pair_recv, xf_send, xf_recv, zf_send, zf_recv,
    dt_send, dt_recv, t_keep, xt_send, xt_recv, gate_col, id_col, w_sem, send_sem, recv_sem,
):
    count, width = tokens.shape
    cap = out_rows.shape[1]
    shards = tok.shape[0]
    me = lax.axis_index("mp")
    z = lax.axis_index("expert")
    core = lax.rem(me, 2)
    over = lax.rem(me + 2, 4)
    mate = me + 1 - 2 * core
    cross = lax.rem(mate + 2, 4)
    pair = z + 1 - 2 * lax.rem(z, 2)
    far = (lax.rem(z + 2, 4), 3 - z)
    to_over, to_mate, to_pair = {"mp": over}, {"mp": mate}, {"expert": pair}
    to_far = ({"expert": far[0]}, {"expert": far[1]})

    loads = []
    for k, (src, dst) in enumerate(((w_ri_h, w_ri), (w_ei_h.at[0], w_ei), (w_eo_h.at[0], w_eo), (w_ro_h, w_ro))):
        load = pltpu.make_async_copy(src, dst, w_sem.at[k])
        load.start()
        loads.append(load)

    barrier = pltpu.get_barrier_semaphore()
    for dest in (to_over, to_mate, to_pair, to_far[0], to_far[1]):
        pl.semaphore_signal(barrier, inc=1, device_id=dest, device_id_type=MESH)

    ids = jnp.where(slot_of[...] >= 0, expert_of[...] * cap + slot_of[...], -1).astype(F32)
    slot_rows = lax.broadcasted_iota(jnp.int32, (cap, count), 0).astype(F32)
    slot_cols = lax.broadcasted_iota(jnp.int32, (count, cap), 1).astype(F32)

    def send_table(e):
        base = (e * cap).astype(F32)
        return jnp.where(slot_rows + base == ids, 1.0, 0.0).astype(BF16)

    def take_table(e):
        base = (e * cap).astype(F32)
        return jnp.where(slot_cols + base == id_col[:, :1], 1.0, 0.0).astype(BF16)

    sent = []

    def send(src, dst, dest):
        k = len(sent)
        copy = pltpu.make_async_remote_copy(
            src_ref=src, dst_ref=dst, send_sem=send_sem.at[k], recv_sem=recv_sem.at[k],
            device_id=dest, device_id_type=MESH,
        )
        copy.start()
        sent.append(copy)
        return copy

    pl.semaphore_wait(barrier, 5)
    tok_over = send(tokens, tok.at[me], to_over)
    tok_mate = send(tokens, tok.at[me], to_mate)
    z_in = []
    for f in range(2):
        out_rows[f + 1] = dot(send_table(far[f]), tokens[...]).astype(BF16)
        z_in.append(send(out_rows.at[f + 1], rows_raw.at[me, f + 1], to_far[f]))
    pair_table = send_table(pair)
    out_rows[0] = dot(pair_table, tokens[...]).astype(BF16)
    pair_in = send(out_rows.at[0], rows_raw.at[me, 0], to_pair)
    tok[me] = tokens[...]
    id_col[...] = jnp.broadcast_to(ids, (128, count)).T
    gate_col[...] = jnp.broadcast_to(gate_prob[...], (128, count)).T

    tok_over.wait_recv()
    tok_cross = send(tok.at[over], tok.at[over], to_mate)
    out_rows2[...] = dot(pair_table, tok[over]).astype(BF16)
    pair_in2 = send(out_rows2, rows_raw.at[over, 0], to_pair)
    x_in, d_in = [], []
    for f in range(2):
        z_in[f].wait_recv()
        piece = rows_raw.at[me, f + 1]
        x_in.append(send(piece, piece, to_over))
        d_in.append(send(piece, piece, to_mate))

    def normalize(load, scale_rows, dst, lo):
        total = 0.0
        for s in range(shards):
            v = load(s).astype(F32)
            total = total + jnp.sum(v * v, axis=-1, keepdims=True)
        inverse = lax.rsqrt(total / (shards * width) + 1e-05)
        for s in range(shards):
            cols = slice(s * width, (s + 1) * width)
            dst[lo:lo + scale_rows, cols] = (load(s).astype(F32) * inverse * gain[:, cols]).astype(BF16)

    tok_mate.wait_recv()
    tok_cross.wait_recv()
    normalize(lambda s: tok[s], count, normed, 0)
    loads[0].wait()
    first_layer(normed, w_ri, res_hid, width)

    pair_in.wait_recv()
    pair_d = send(rows_raw.at[me, 0], rows_raw.at[me, 0], to_mate)
    pair_in2.wait_recv()
    pair_d2 = send(rows_raw.at[over, 0], rows_raw.at[over, 0], to_mate)
    rows_near[:cap, :] = dot(send_table(z), normed[...]).astype(BF16)
    pair_d.wait_recv()
    pair_d2.wait_recv()
    normalize(lambda s: rows_raw[s, 0], cap, rows_near, cap)
    loads[1].wait()
    first_layer(rows_near, w_ei, hid, width)

    d_in2 = []
    for f in range(2):
        x_in[f].wait_recv()
        piece = rows_raw.at[over, f + 1]
        d_in2.append(send(piece, piece, to_mate))

    loads[2].wait()

    def shard_cols(s):
        return pl.ds(pl.multiple_of(s * width, width), width)

    de = []
    for j, s in enumerate((mate, cross)):
        part = dot(hid[...], w_eo[:, shard_cols(s)])
        own_part[s] = part[:cap].astype(BF16)
        de_send[j, 0] = part[cap:].astype(BF16)
        de.append(send(de_send.at[j, 0], de_recv.at[j, 0], to_mate))
    for j, s in enumerate((me, over)):
        part = dot(hid[...], w_eo[:, shard_cols(s)])
        own_part[s] = part[:cap].astype(BF16)
        e_keep[j, 0] = part[cap:]

    pair_out = []
    for j in range(2):
        de[j].wait_recv()
        pair_send[j] = (e_keep[j, 0] + de_recv[j, 0].astype(F32)).astype(BF16)
        pair_out.append(send(pair_send.at[j], pair_recv.at[j], to_pair))

    for f in range(2):
        d_in[f].wait_recv()
        d_in2[f].wait_recv()
        normalize(lambda s, f=f: rows_raw[s, f + 1], cap, rows_far, f * cap)
    first_layer(rows_far, w_ei, hid, width)
    de_far = {}
    for j, s in ((1, cross), (0, mate)):
        part = dot(hid[...], w_eo[:, shard_cols(s)])
        for f in range(2):
            de_send[j, f + 1] = part[f * cap:(f + 1) * cap].astype(BF16)
            de_far[j, f] = send(de_send.at[j, f + 1], de_recv.at[j, f + 1], to_mate)
    for j, s in ((1, over), (0, me)):
        part = dot(hid[...], w_eo[:, shard_cols(s)])
        for f in range(2):
            e_keep[j, f + 1] = part[f * cap:(f + 1) * cap]
    xf = []
    for f in range(2):
        de_far[1, f].wait_recv()
        xf_send[f] = (e_keep[1, f + 1] + de_recv[1, f + 1].astype(F32)).astype(BF16)
        xf.append(send(xf_send.at[f], xf_recv.at[f], to_over))

    loads[3].wait()
    own_take = take_table(z)
    dt = {}

    def token_part(s):
        return dot(res_hid[...], w_ro[:, shard_cols(s)]) + gate_col[:, :1] * dot(own_take, own_part[s])

    for j, s in ((1, cross), (0, mate)):
        dt_send[j] = token_part(s).astype(BF16)
        dt[j] = send(dt_send.at[j], dt_recv.at[j], to_mate)
    for j, s in ((1, over), (0, me)):
        t_keep[j] = token_part(s)

    pair_take = take_table(pair)

    def chip_sum(j):
        pair_out[j].wait_recv()
        dt[j].wait_recv()
        return t_keep[j] + dt_recv[j].astype(F32) + gate_col[:, :1] * dot(pair_take, pair_recv[j])

    xt_send[...] = chip_sum(1).astype(BF16)
    xt = send(xt_send, xt_recv, to_over)
    zf = []
    for f in range(2):
        xf[f].wait_recv()
        de_far[0, f].wait_recv()
        full = e_keep[0, f + 1] + de_recv[0, f + 1].astype(F32) + xf_recv[f].astype(F32)
        zf_send[f] = full.astype(BF16)
        zf.append(send(zf_send.at[f], zf_recv.at[f], to_far[f]))
    t_keep[0] = chip_sum(0)
    for f in range(2):
        zf[f].wait_recv()
        t_keep[0] = t_keep[0] + gate_col[:, :1] * dot(take_table(far[f]), zf_recv[f])
    xt.wait_recv()
    out[...] = (t_keep[0] + xt_recv[...].astype(F32)).astype(BF16)
    for copy in sent:
        copy.wait_send()


def fused(tokens, gain, w_res_in, w_res_out, w_exp_in, w_exp_out, expert_of, slot_of, gate_prob):
    count, width = tokens.shape
    shards = lax.axis_size("mp")
    experts = lax.axis_size("expert")
    cap = max(2, 5 * count // (4 * experts))
    model, hidden = w_res_in.shape
    exp_hidden = w_exp_in.shape[2]
    vmem, hbm = pl.BlockSpec(memory_space=pltpu.VMEM), pl.BlockSpec(memory_space=pl.ANY)
    buf = lambda *shape: pltpu.VMEM(shape, BF16)
    wide = lambda *shape: pltpu.VMEM(shape, F32)
    copies = 30
    return pl.pallas_call(
        fused_kernel,
        out_shape=jax.ShapeDtypeStruct((count, width), BF16),
        in_specs=[vmem, vmem, hbm, hbm, hbm, hbm, vmem, vmem, vmem],
        out_specs=vmem,
        scratch_shapes=[
            buf(model, hidden), buf(hidden, model), buf(model, exp_hidden), buf(exp_hidden, model),
            buf(shards, count, width), buf(count, model), buf(count, hidden),
            buf(shards, 3, cap, width), buf(3, cap, width), buf(cap, width),
            buf(2 * cap, model), buf(2 * cap, model), buf(2 * cap, exp_hidden),
            buf(shards, cap, width), buf(2, 3, cap, width), buf(2, 3, cap, width), wide(2, 3, cap, width),
            buf(2, cap, width), buf(2, cap, width), buf(2, cap, width), buf(2, cap, width),
            buf(2, cap, width), buf(2, cap, width),
            buf(2, count, width), buf(2, count, width), wide(2, count, width),
            buf(count, width), buf(count, width), wide(count, 128), wide(count, 128),
            pltpu.SemaphoreType.DMA((4,)), pltpu.SemaphoreType.DMA((copies,)), pltpu.SemaphoreType.DMA((copies,)),
        ],
        name="fused_layer",
        compiler_params=pltpu.CompilerParams(
            collective_id=0, has_side_effects=True, vmem_limit_bytes=56 * 1024 * 1024
        ),
    )(
        tokens, gain[None, :], w_res_in, w_res_out, w_exp_in, w_exp_out,
        expert_of[None, :], slot_of[None, :], gate_prob[None, :],
    )


def pick(mesh):
    if mesh.shape["mp"] == 4 and mesh.shape["expert"] == 4:
        return fused
    return per_device


def solution(mesh):
    return jax.shard_map(
        pick(mesh),
        mesh=mesh,
        in_specs=(
            P(("groups", "expert"), "mp"),
            P(),
            P(None, "mp"),
            P("mp", None),
            P("expert", None, "mp"),
            P("expert", "mp", None),
            P(("groups", "expert")),
            P(("groups", "expert")),
            P(("groups", "expert")),
        ),
        out_specs=P(("groups", "expert"), "mp"),
        check_vma=False,
    )
```

```python
import functools

import jax
import jax.numpy as jnp
from jax import lax
from jax.experimental import pallas as pl
from jax.experimental.pallas import tpu as pltpu
from jax.sharding import PartitionSpec as P


def rms_rows(tokens, gain):
    values = tokens.astype(jnp.float32)
    inverse = lax.rsqrt(jnp.mean(values * values, axis=-1, keepdims=True) + 1e-05)
    return (values * inverse * gain).astype(jnp.bfloat16)


def per_device(
    tokens, gain, w_res_in, w_res_out, w_exp_in, w_exp_out, expert_of, slot_of, gate_prob
):
    full_rows = lax.all_gather(tokens, "mp", axis=1, tiled=True)
    normed = rms_rows(full_rows, gain)
    res_hidden = jax.nn.gelu(jnp.dot(normed, w_res_in, preferred_element_type=jnp.float32)).astype(
        jnp.bfloat16
    )
    res_part = jnp.dot(res_hidden, w_res_out, preferred_element_type=jnp.float32)
    row_count = expert_of.shape[0]
    experts = lax.axis_size("expert")
    capacity = max(2, 5 * row_count // (4 * experts))
    feat_width = tokens.shape[1]
    slot_id = jnp.where(slot_of >= 0, expert_of * capacity + slot_of, -1)
    slot_index = jnp.arange(experts * capacity, dtype=jnp.int32)
    send_table = (slot_index[:, None] == slot_id[None, :]).astype(jnp.bfloat16)
    take_table = (slot_id[:, None] == slot_index[None, :]).astype(jnp.bfloat16)
    local_in = w_exp_in[0]
    local_out = w_exp_out[0]
    mp_index = lax.axis_index("mp")
    own_slice = lax.dynamic_slice_in_dim(normed, mp_index * feat_width, feat_width, 1)
    outgoing = jnp.dot(send_table, own_slice, preferred_element_type=jnp.float32).astype(
        jnp.bfloat16
    )
    incoming = lax.all_to_all(
        outgoing.reshape(experts, capacity, feat_width),
        "expert",
        split_axis=0,
        concat_axis=0,
        tiled=True,
    )
    piece = lax.all_gather(incoming, "mp", axis=2, tiled=True)
    flat_piece = piece.reshape(-1, piece.shape[2])
    preact = jnp.dot(flat_piece, local_in, preferred_element_type=jnp.float32)
    exp_hidden = jax.nn.gelu(preact).astype(jnp.bfloat16)
    exp_part = jnp.dot(exp_hidden, local_out, preferred_element_type=jnp.float32)
    gate_column = gate_prob[:, None]
    summed = lax.psum_scatter(exp_part.astype(jnp.bfloat16), "mp", scatter_dimension=1, tiled=True)
    returned = lax.all_to_all(
        summed.reshape(experts, capacity, feat_width),
        "expert",
        split_axis=0,
        concat_axis=0,
        tiled=True,
    )
    moe_value = jnp.dot(
        take_table,
        returned.reshape(experts * capacity, feat_width),
        preferred_element_type=jnp.float32,
    )
    res_sum = lax.psum_scatter(
        res_part.astype(jnp.bfloat16), "mp", scatter_dimension=1, tiled=True
    ).astype(jnp.float32)
    return (res_sum + gate_column * moe_value).astype(jnp.bfloat16)


MESH = pl.DeviceIdType.MESH
F32 = jnp.float32
BF16 = jnp.bfloat16


def dot(a, b):
    return jnp.dot(a, b, preferred_element_type=F32)


def first_layer(rows_ref, w_ref, hidden_ref, chunk, lo, size):
    def body(n, carry):
        cols = pl.ds(pl.multiple_of(n * chunk, chunk), chunk)
        hidden_ref[lo:lo + size, cols] = jax.nn.gelu(dot(rows_ref[lo:lo + size], w_ref[:, cols])).astype(BF16)
        return carry

    lax.fori_loop(0, hidden_ref.shape[1] // chunk, body, 0)


def fused_kernel(
    halves, tokens, gain, w_ri_h, w_ro_h, w_ei_h, w_eo_h, expert_of, slot_of, gate_prob, out,
    w_ri, w_ro, w_ei, w_eo, tok, normed, res_hid, rows_raw, out_rows, out_rows2, rows_near, rows_far,
    hid_near, hid, own_part, de_send, de_recv, e_keep, pair_send, pair_recv, xf_send, xf_recv, zf_send, zf_recv,
    dt_send, dt_recv, t_keep, xt_send, xt_recv, gate_col, id_col, w_sem, send_sem, recv_sem,
):
    count, width = tokens.shape
    cap = out_rows.shape[1]
    shards = tok.shape[0]
    me = lax.axis_index("mp")
    z = lax.axis_index("expert")
    core = lax.rem(me, 2)
    over = lax.rem(me + 2, 4)
    mate = me + 1 - 2 * core
    cross = lax.rem(mate + 2, 4)
    pair = z + 1 - 2 * lax.rem(z, 2)
    far = (lax.rem(z + 2, 4), 3 - z)
    to_over, to_mate, to_pair = {"mp": over}, {"mp": mate}, {"expert": pair}
    to_far = ({"expert": far[0]}, {"expert": far[1]})

    loads = []
    for k, (src, dst) in enumerate(((w_ri_h, w_ri), (w_ei_h.at[0], w_ei), (w_eo_h.at[0], w_eo), (w_ro_h, w_ro))):
        load = pltpu.make_async_copy(src, dst, w_sem.at[k])
        load.start()
        loads.append(load)

    barrier = pltpu.get_barrier_semaphore()
    for dest in (to_over, to_mate, to_pair, to_far[0], to_far[1]):
        pl.semaphore_signal(barrier, inc=1, device_id=dest, device_id_type=MESH)

    ids = jnp.where(slot_of[...] >= 0, expert_of[...] * cap + slot_of[...], -1).astype(F32)
    slot_rows = lax.broadcasted_iota(jnp.int32, (cap, count), 0).astype(F32)
    slot_cols = lax.broadcasted_iota(jnp.int32, (count, cap), 1).astype(F32)

    def send_table(e):
        base = (e * cap).astype(F32)
        return jnp.where(slot_rows + base == ids, 1.0, 0.0).astype(BF16)

    def take_table(e):
        base = (e * cap).astype(F32)
        return jnp.where(slot_cols + base == id_col[:, :1], 1.0, 0.0).astype(BF16)

    sent = []

    def send(src, dst, dest):
        k = len(sent)
        copy = pltpu.make_async_remote_copy(
            src_ref=src, dst_ref=dst, send_sem=send_sem.at[k], recv_sem=recv_sem.at[k],
            device_id=dest, device_id_type=MESH,
        )
        copy.start()
        sent.append(copy)
        return copy

    pl.semaphore_wait(barrier, 5)
    half = count // halves
    spans = [slice(h * half, (h + 1) * half) for h in range(halves)]
    tok_over = [send(tokens.at[r], tok.at[me, r], to_over) for r in spans]
    tok_mate = send(tokens, tok.at[me], to_mate)
    z_in = []
    for f in range(2):
        out_rows[f + 1] = dot(send_table(far[f]), tokens[...]).astype(BF16)
        z_in.append(send(out_rows.at[f + 1], rows_raw.at[me, f + 1], to_far[f]))
    pair_table = send_table(pair)
    out_rows[0] = dot(pair_table, tokens[...]).astype(BF16)
    pair_in = send(out_rows.at[0], rows_raw.at[me, 0], to_pair)
    tok[me] = tokens[...]
    id_col[...] = jnp.broadcast_to(ids, (128, count)).T
    gate_col[...] = jnp.broadcast_to(gate_prob[...], (128, count)).T

    def normalize(load, scale_rows, dst, lo):
        total = 0.0
        for s in range(shards):
            v = load(s).astype(F32)
            total = total + jnp.sum(v * v, axis=-1, keepdims=True)
        inverse = lax.rsqrt(total / (shards * width) + 1e-05)
        for s in range(shards):
            cols = slice(s * width, (s + 1) * width)
            dst[lo:lo + scale_rows, cols] = (load(s).astype(F32) * inverse * gain[:, cols]).astype(BF16)


    def shard_cols(s):
        return pl.ds(pl.multiple_of(s * width, width), width)

    tok_cross = []

    def relay(h):
        tok_over[h].wait_recv()
        piece = tok.at[over, spans[h]]
        tok_cross.append(send(piece, piece, to_mate))

    def residual(h):
        r = spans[h]
        tok_cross[h].wait_recv()
        normalize(lambda s: tok[s, r], half, normed, h * half)
        first_layer(normed, w_ri, res_hid, width, h * half, half)

    relay(0)
    tok_mate.wait_recv()
    loads[0].wait()
    for h in range(halves - 1):
        residual(h)
        relay(h + 1)
    out_rows2[...] = dot(pair_table, tok[over]).astype(BF16)
    pair_in2 = send(out_rows2, rows_raw.at[over, 0], to_pair)
    x_in, d_in = [], []
    for f in range(2):
        z_in[f].wait_recv()
        piece = rows_raw.at[me, f + 1]
        x_in.append(send(piece, piece, to_over))
        d_in.append(send(piece, piece, to_mate))
    residual(halves - 1)

    pair_in.wait_recv()
    pair_d = send(rows_raw.at[me, 0], rows_raw.at[me, 0], to_mate)
    pair_in2.wait_recv()
    pair_d2 = send(rows_raw.at[over, 0], rows_raw.at[over, 0], to_mate)
    rows_near[:cap, :] = dot(send_table(z), normed[...]).astype(BF16)
    pair_d.wait_recv()
    pair_d2.wait_recv()
    normalize(lambda s: rows_raw[s, 0], cap, rows_near, cap)
    loads[1].wait()
    first_layer(rows_near, w_ei, hid_near, width, 0, 2 * cap)

    d_in2 = []
    for f in range(2):
        x_in[f].wait_recv()
        piece = rows_raw.at[over, f + 1]
        d_in2.append(send(piece, piece, to_mate))
    loads[2].wait()
    for f in range(2):
        d_in[f].wait_recv()
        d_in2[f].wait_recv()
        normalize(lambda s, f=f: rows_raw[s, f + 1], cap, rows_far, f * cap)
    first_layer(rows_far, w_ei, hid, width, 0, 2 * cap)
    de_far, xf = {}, []

    def far_give(j, s):
        part = dot(hid[...], w_eo[:, shard_cols(s)])
        for f in range(2):
            de_send[j, f + 1] = part[f * cap:(f + 1) * cap].astype(BF16)
            de_far[j, f] = send(de_send.at[j, f + 1], de_recv.at[j, f + 1], to_mate)

    def far_keep(j, s):
        part = dot(hid[...], w_eo[:, shard_cols(s)])
        for f in range(2):
            e_keep[j, f + 1] = part[f * cap:(f + 1) * cap]

    far_give(1, cross)
    far_keep(1, over)
    far_give(0, mate)
    for f in range(2):
        de_far[1, f].wait_recv()
        xf_send[f] = (e_keep[1, f + 1] + de_recv[1, f + 1].astype(F32)).astype(BF16)
        xf.append(send(xf_send.at[f], xf_recv.at[f], to_over))
    far_keep(0, me)

    de = {}
    for j, s in ((1, cross), (0, mate)):
        part = dot(hid_near[...], w_eo[:, shard_cols(s)])
        own_part[s] = part[:cap].astype(BF16)
        de_send[j, 0] = part[cap:].astype(BF16)
        de[j] = send(de_send.at[j, 0], de_recv.at[j, 0], to_mate)
    for j, s in ((1, over), (0, me)):
        part = dot(hid_near[...], w_eo[:, shard_cols(s)])
        own_part[s] = part[:cap].astype(BF16)
        e_keep[j, 0] = part[cap:]
    pair_out = {}
    for j in (1, 0):
        de[j].wait_recv()
        pair_send[j] = (e_keep[j, 0] + de_recv[j, 0].astype(F32)).astype(BF16)
        pair_out[j] = send(pair_send.at[j], pair_recv.at[j], to_pair)

    loads[3].wait()
    own_take = take_table(z)
    pair_take = take_table(pair)
    dt = {}

    def token_part(s):
        return dot(res_hid[...], w_ro[:, shard_cols(s)]) + gate_col[:, :1] * dot(own_take, own_part[s])

    def token_give(j, s):
        dt_send[j] = token_part(s).astype(BF16)
        dt[j] = send(dt_send.at[j], dt_recv.at[j], to_mate)

    def chip_sum(j):
        pair_out[j].wait_recv()
        dt[j].wait_recv()
        return t_keep[j] + dt_recv[j].astype(F32) + gate_col[:, :1] * dot(pair_take, pair_recv[j])

    zf = []

    def far_home(f):
        xf[f].wait_recv()
        de_far[0, f].wait_recv()
        full = e_keep[0, f + 1] + de_recv[0, f + 1].astype(F32) + xf_recv[f].astype(F32)
        zf_send[f] = full.astype(BF16)
        zf.append(send(zf_send.at[f], zf_recv.at[f], to_far[f]))

    token_give(1, cross)
    t_keep[1] = token_part(over)
    far_home(0)
    xt_send[...] = chip_sum(1).astype(BF16)
    xt = send(xt_send, xt_recv, to_over)
    far_home(1)
    token_give(0, mate)
    t_keep[0] = token_part(me)
    t_keep[0] = chip_sum(0)
    for f in range(2):
        far_take = take_table(far[f])
        zf[f].wait_recv()
        t_keep[0] = t_keep[0] + gate_col[:, :1] * dot(far_take, zf_recv[f])
    xt.wait_recv()
    out[...] = (t_keep[0] + xt_recv[...].astype(F32)).astype(BF16)
    for copy in sent:
        copy.wait_send()


def fused(tokens, gain, w_res_in, w_res_out, w_exp_in, w_exp_out, expert_of, slot_of, gate_prob):
    count, width = tokens.shape
    shards = lax.axis_size("mp")
    experts = lax.axis_size("expert")
    cap = max(2, 5 * count // (4 * experts))
    model, hidden = w_res_in.shape
    exp_hidden = w_exp_in.shape[2]
    vmem, hbm = pl.BlockSpec(memory_space=pltpu.VMEM), pl.BlockSpec(memory_space=pl.ANY)
    buf = lambda *shape: pltpu.VMEM(shape, BF16)
    wide = lambda *shape: pltpu.VMEM(shape, F32)
    halves = 2
    copies = 28 + 2 * halves
    return pl.pallas_call(
        functools.partial(fused_kernel, halves),
        out_shape=jax.ShapeDtypeStruct((count, width), BF16),
        in_specs=[vmem, vmem, hbm, hbm, hbm, hbm, vmem, vmem, vmem],
        out_specs=vmem,
        scratch_shapes=[
            buf(model, hidden), buf(hidden, model), buf(model, exp_hidden), buf(exp_hidden, model),
            buf(shards, count, width), buf(count, model), buf(count, hidden),
            buf(shards, 3, cap, width), buf(3, cap, width), buf(cap, width),
            buf(2 * cap, model), buf(2 * cap, model), buf(2 * cap, exp_hidden), buf(2 * cap, exp_hidden),
            buf(shards, cap, width), buf(2, 3, cap, width), buf(2, 3, cap, width), wide(2, 3, cap, width),
            buf(2, cap, width), buf(2, cap, width), buf(2, cap, width), buf(2, cap, width),
            buf(2, cap, width), buf(2, cap, width),
            buf(2, count, width), buf(2, count, width), wide(2, count, width),
            buf(count, width), buf(count, width), wide(count, 128), wide(count, 128),
            pltpu.SemaphoreType.DMA((4,)), pltpu.SemaphoreType.DMA((copies,)), pltpu.SemaphoreType.DMA((copies,)),
        ],
        name="fused_layer",
        compiler_params=pltpu.CompilerParams(
            collective_id=0, has_side_effects=True, vmem_limit_bytes=56 * 1024 * 1024
        ),
    )(
        tokens, gain[None, :], w_res_in, w_res_out, w_exp_in, w_exp_out,
        expert_of[None, :], slot_of[None, :], gate_prob[None, :],
    )


def pick(mesh):
    if mesh.shape["mp"] == 4 and mesh.shape["expert"] == 4:
        return fused
    return per_device


def solution(mesh):
    return jax.shard_map(
        pick(mesh),
        mesh=mesh,
        in_specs=(
            P(("groups", "expert"), "mp"),
            P(),
            P(None, "mp"),
            P("mp", None),
            P("expert", None, "mp"),
            P("expert", "mp", None),
            P(("groups", "expert")),
            P(("groups", "expert")),
            P(("groups", "expert")),
        ),
        out_specs=P(("groups", "expert"), "mp"),
        check_vma=False,
    )
```

```python
import functools

import jax
import jax.numpy as jnp
from jax import lax
from jax.experimental import pallas as pl
from jax.experimental.pallas import tpu as pltpu
from jax.sharding import PartitionSpec as P


def rms_rows(tokens, gain):
    values = tokens.astype(jnp.float32)
    inverse = lax.rsqrt(jnp.mean(values * values, axis=-1, keepdims=True) + 1e-05)
    return (values * inverse * gain).astype(jnp.bfloat16)


def per_device(
    tokens, gain, w_res_in, w_res_out, w_exp_in, w_exp_out, expert_of, slot_of, gate_prob
):
    full_rows = lax.all_gather(tokens, "mp", axis=1, tiled=True)
    normed = rms_rows(full_rows, gain)
    res_hidden = jax.nn.gelu(jnp.dot(normed, w_res_in, preferred_element_type=jnp.float32)).astype(
        jnp.bfloat16
    )
    res_part = jnp.dot(res_hidden, w_res_out, preferred_element_type=jnp.float32)
    row_count = expert_of.shape[0]
    experts = lax.axis_size("expert")
    capacity = max(2, 5 * row_count // (4 * experts))
    feat_width = tokens.shape[1]
    slot_id = jnp.where(slot_of >= 0, expert_of * capacity + slot_of, -1)
    slot_index = jnp.arange(experts * capacity, dtype=jnp.int32)
    send_table = (slot_index[:, None] == slot_id[None, :]).astype(jnp.bfloat16)
    take_table = (slot_id[:, None] == slot_index[None, :]).astype(jnp.bfloat16)
    local_in = w_exp_in[0]
    local_out = w_exp_out[0]
    mp_index = lax.axis_index("mp")
    own_slice = lax.dynamic_slice_in_dim(normed, mp_index * feat_width, feat_width, 1)
    outgoing = jnp.dot(send_table, own_slice, preferred_element_type=jnp.float32).astype(
        jnp.bfloat16
    )
    incoming = lax.all_to_all(
        outgoing.reshape(experts, capacity, feat_width),
        "expert",
        split_axis=0,
        concat_axis=0,
        tiled=True,
    )
    piece = lax.all_gather(incoming, "mp", axis=2, tiled=True)
    flat_piece = piece.reshape(-1, piece.shape[2])
    preact = jnp.dot(flat_piece, local_in, preferred_element_type=jnp.float32)
    exp_hidden = jax.nn.gelu(preact).astype(jnp.bfloat16)
    exp_part = jnp.dot(exp_hidden, local_out, preferred_element_type=jnp.float32)
    gate_column = gate_prob[:, None]
    summed = lax.psum_scatter(exp_part.astype(jnp.bfloat16), "mp", scatter_dimension=1, tiled=True)
    returned = lax.all_to_all(
        summed.reshape(experts, capacity, feat_width),
        "expert",
        split_axis=0,
        concat_axis=0,
        tiled=True,
    )
    moe_value = jnp.dot(
        take_table,
        returned.reshape(experts * capacity, feat_width),
        preferred_element_type=jnp.float32,
    )
    res_sum = lax.psum_scatter(
        res_part.astype(jnp.bfloat16), "mp", scatter_dimension=1, tiled=True
    ).astype(jnp.float32)
    return (res_sum + gate_column * moe_value).astype(jnp.bfloat16)


MESH = pl.DeviceIdType.MESH
F32 = jnp.float32
BF16 = jnp.bfloat16


def dot(a, b):
    return jnp.dot(a, b, preferred_element_type=F32)


def first_layer(rows_ref, w_ref, hidden_ref, chunk, lo, size):
    def body(n, carry):
        cols = pl.ds(pl.multiple_of(n * chunk, chunk), chunk)
        hidden_ref[lo:lo + size, cols] = jax.nn.gelu(dot(rows_ref[lo:lo + size], w_ref[:, cols])).astype(BF16)
        return carry

    lax.fori_loop(0, hidden_ref.shape[1] // chunk, body, 0)


def fused_kernel(
    halves, tokens, gain, w_ri_h, w_ro_h, w_ei_h, w_eo_h, expert_of, slot_of, gate_prob, out,
    w_ri, w_ro, w_ei, w_eo, tok, normed, res_hid, rows_raw, out_rows, out_rows2, rows_near, rows_far,
    hid_near, hid, own_part, de_send, de_recv, e_keep, pair_send, pair_recv, xf_send, xf_recv, zf_send, zf_recv,
    dt_send, dt_recv, t_keep, xt_send, xt_recv, gate_col, id_col, w_sem, send_sem, recv_sem,
):
    count, width = tokens.shape
    cap = out_rows.shape[1]
    shards = tok.shape[0]
    me = lax.axis_index("mp")
    z = lax.axis_index("expert")
    core = lax.rem(me, 2)
    over = lax.rem(me + 2, 4)
    mate = me + 1 - 2 * core
    cross = lax.rem(mate + 2, 4)
    pair = z + 1 - 2 * lax.rem(z, 2)
    far = (lax.rem(z + 2, 4), 3 - z)
    to_over, to_mate, to_pair = {"mp": over}, {"mp": mate}, {"expert": pair}
    to_far = ({"expert": far[0]}, {"expert": far[1]})

    loads = []
    for k, (src, dst) in enumerate(((w_ri_h, w_ri), (w_ei_h.at[0], w_ei), (w_eo_h.at[0], w_eo), (w_ro_h, w_ro))):
        load = pltpu.make_async_copy(src, dst, w_sem.at[k])
        load.start()
        loads.append(load)

    barrier = pltpu.get_barrier_semaphore()
    for dest in (to_over, to_mate, to_pair, to_far[0], to_far[1]):
        pl.semaphore_signal(barrier, inc=1, device_id=dest, device_id_type=MESH)

    ids = jnp.where(slot_of[...] >= 0, expert_of[...] * cap + slot_of[...], -1).astype(F32)
    slot_rows = lax.broadcasted_iota(jnp.int32, (cap, count), 0).astype(F32)
    slot_cols = lax.broadcasted_iota(jnp.int32, (count, cap), 1).astype(F32)

    def send_table(e):
        base = (e * cap).astype(F32)
        return jnp.where(slot_rows + base == ids, 1.0, 0.0).astype(BF16)

    def take_table(e):
        base = (e * cap).astype(F32)
        return jnp.where(slot_cols + base == id_col[:, :1], 1.0, 0.0).astype(BF16)

    sent = []

    def send(src, dst, dest):
        k = len(sent)
        copy = pltpu.make_async_remote_copy(
            src_ref=src, dst_ref=dst, send_sem=send_sem.at[k], recv_sem=recv_sem.at[k],
            device_id=dest, device_id_type=MESH,
        )
        copy.start()
        sent.append(copy)
        return copy

    pl.semaphore_wait(barrier, 5)
    half = count // halves
    spans = [slice(h * half, (h + 1) * half) for h in range(halves)]
    tok_over = [send(tokens.at[r], tok.at[me, r], to_over) for r in spans]
    tok_mate = send(tokens, tok.at[me], to_mate)
    z_in = []
    for f in range(2):
        out_rows[f + 1] = dot(send_table(far[f]), tokens[...]).astype(BF16)
        z_in.append(send(out_rows.at[f + 1], rows_raw.at[me, f + 1], to_far[f]))
    pair_table = send_table(pair)
    out_rows[0] = dot(pair_table, tokens[...]).astype(BF16)
    pair_in = send(out_rows.at[0], rows_raw.at[me, 0], to_pair)
    tok[me] = tokens[...]
    id_col[...] = jnp.broadcast_to(ids, (128, count)).T
    gate_col[...] = jnp.broadcast_to(gate_prob[...], (128, count)).T

    def normalize(load, scale_rows, dst, lo):
        total = 0.0
        for s in range(shards):
            v = load(s).astype(F32)
            total = total + jnp.sum(v * v, axis=-1, keepdims=True)
        inverse = lax.rsqrt(total / (shards * width) + 1e-05)
        for s in range(shards):
            cols = slice(s * width, (s + 1) * width)
            dst[lo:lo + scale_rows, cols] = (load(s).astype(F32) * inverse * gain[:, cols]).astype(BF16)


    def shard_cols(s):
        return pl.ds(pl.multiple_of(s * width, width), width)

    tok_cross = []

    def relay(h):
        tok_over[h].wait_recv()
        piece = tok.at[over, spans[h]]
        tok_cross.append(send(piece, piece, to_mate))

    def residual(h):
        r = spans[h]
        tok_cross[h].wait_recv()
        normalize(lambda s: tok[s, r], half, normed, h * half)
        first_layer(normed, w_ri, res_hid, width, h * half, half)

    relay(0)
    tok_mate.wait_recv()
    loads[0].wait()
    for h in range(halves - 1):
        residual(h)
        relay(h + 1)
    out_rows2[...] = dot(pair_table, tok[over]).astype(BF16)
    pair_in2 = send(out_rows2, rows_raw.at[over, 0], to_pair)
    x_in, d_in = [], []
    for f in range(2):
        z_in[f].wait_recv()
        piece = rows_raw.at[me, f + 1]
        x_in.append(send(piece, piece, to_over))
        d_in.append(send(piece, piece, to_mate))
    residual(halves - 1)

    pair_in.wait_recv()
    pair_d = send(rows_raw.at[me, 0], rows_raw.at[me, 0], to_mate)
    pair_in2.wait_recv()
    pair_d2 = send(rows_raw.at[over, 0], rows_raw.at[over, 0], to_mate)
    rows_near[:cap, :] = dot(send_table(z), normed[...]).astype(BF16)
    pair_d.wait_recv()
    pair_d2.wait_recv()
    normalize(lambda s: rows_raw[s, 0], cap, rows_near, cap)
    loads[1].wait()
    first_layer(rows_near, w_ei, hid_near, width, 0, 2 * cap)

    d_in2 = []
    for f in range(2):
        x_in[f].wait_recv()
        piece = rows_raw.at[over, f + 1]
        d_in2.append(send(piece, piece, to_mate))
    loads[2].wait()
    de = {}
    for j, s in ((1, cross), (0, mate)):
        part = dot(hid_near[...], w_eo[:, shard_cols(s)])
        own_part[s] = part[:cap].astype(BF16)
        de_send[j, 0] = part[cap:].astype(BF16)
        de[j] = send(de_send.at[j, 0], de_recv.at[j, 0], to_mate)
    for j, s in ((1, over), (0, me)):
        part = dot(hid_near[...], w_eo[:, shard_cols(s)])
        own_part[s] = part[:cap].astype(BF16)
        e_keep[j, 0] = part[cap:]
    pair_out = {}
    for j in (1, 0):
        de[j].wait_recv()
        pair_send[j] = (e_keep[j, 0] + de_recv[j, 0].astype(F32)).astype(BF16)
        pair_out[j] = send(pair_send.at[j], pair_recv.at[j], to_pair)

    for f in range(2):
        d_in[f].wait_recv()
        d_in2[f].wait_recv()
        normalize(lambda s, f=f: rows_raw[s, f + 1], cap, rows_far, f * cap)
    first_layer(rows_far, w_ei, hid, width, 0, 2 * cap)
    de_far, xf = {}, []

    def far_give(j, s):
        part = dot(hid[...], w_eo[:, shard_cols(s)])
        for f in range(2):
            de_send[j, f + 1] = part[f * cap:(f + 1) * cap].astype(BF16)
            de_far[j, f] = send(de_send.at[j, f + 1], de_recv.at[j, f + 1], to_mate)

    def far_keep(j, s):
        part = dot(hid[...], w_eo[:, shard_cols(s)])
        for f in range(2):
            e_keep[j, f + 1] = part[f * cap:(f + 1) * cap]

    far_give(1, cross)
    far_keep(1, over)
    far_give(0, mate)
    for f in range(2):
        de_far[1, f].wait_recv()
        xf_send[f] = (e_keep[1, f + 1] + de_recv[1, f + 1].astype(F32)).astype(BF16)
        xf.append(send(xf_send.at[f], xf_recv.at[f], to_over))
    far_keep(0, me)

    loads[3].wait()
    own_take = take_table(z)
    pair_take = take_table(pair)
    dt = {}

    def token_part(s):
        return dot(res_hid[...], w_ro[:, shard_cols(s)]) + gate_col[:, :1] * dot(own_take, own_part[s])

    def token_give(j, s):
        dt_send[j] = token_part(s).astype(BF16)
        dt[j] = send(dt_send.at[j], dt_recv.at[j], to_mate)

    def chip_sum(j):
        pair_out[j].wait_recv()
        dt[j].wait_recv()
        return t_keep[j] + dt_recv[j].astype(F32) + gate_col[:, :1] * dot(pair_take, pair_recv[j])

    zf = []

    def far_home(f):
        xf[f].wait_recv()
        de_far[0, f].wait_recv()
        full = e_keep[0, f + 1] + de_recv[0, f + 1].astype(F32) + xf_recv[f].astype(F32)
        zf_send[f] = full.astype(BF16)
        zf.append(send(zf_send.at[f], zf_recv.at[f], to_far[f]))

    token_give(1, cross)
    t_keep[1] = token_part(over)
    far_home(0)
    xt_send[...] = chip_sum(1).astype(BF16)
    xt = send(xt_send, xt_recv, to_over)
    far_home(1)
    token_give(0, mate)
    t_keep[0] = token_part(me)
    t_keep[0] = chip_sum(0)
    for f in range(2):
        far_take = take_table(far[f])
        zf[f].wait_recv()
        t_keep[0] = t_keep[0] + gate_col[:, :1] * dot(far_take, zf_recv[f])
    xt.wait_recv()
    out[...] = (t_keep[0] + xt_recv[...].astype(F32)).astype(BF16)
    for copy in sent:
        copy.wait_send()


def fused(tokens, gain, w_res_in, w_res_out, w_exp_in, w_exp_out, expert_of, slot_of, gate_prob):
    count, width = tokens.shape
    shards = lax.axis_size("mp")
    experts = lax.axis_size("expert")
    cap = max(2, 5 * count // (4 * experts))
    model, hidden = w_res_in.shape
    exp_hidden = w_exp_in.shape[2]
    vmem, hbm = pl.BlockSpec(memory_space=pltpu.VMEM), pl.BlockSpec(memory_space=pl.ANY)
    buf = lambda *shape: pltpu.VMEM(shape, BF16)
    wide = lambda *shape: pltpu.VMEM(shape, F32)
    halves = 2
    copies = 28 + 2 * halves
    return pl.pallas_call(
        functools.partial(fused_kernel, halves),
        out_shape=jax.ShapeDtypeStruct((count, width), BF16),
        in_specs=[vmem, vmem, hbm, hbm, hbm, hbm, vmem, vmem, vmem],
        out_specs=vmem,
        scratch_shapes=[
            buf(model, hidden), buf(hidden, model), buf(model, exp_hidden), buf(exp_hidden, model),
            buf(shards, count, width), buf(count, model), buf(count, hidden),
            buf(shards, 3, cap, width), buf(3, cap, width), buf(cap, width),
            buf(2 * cap, model), buf(2 * cap, model), buf(2 * cap, exp_hidden), buf(2 * cap, exp_hidden),
            buf(shards, cap, width), buf(2, 3, cap, width), buf(2, 3, cap, width), wide(2, 3, cap, width),
            buf(2, cap, width), buf(2, cap, width), buf(2, cap, width), buf(2, cap, width),
            buf(2, cap, width), buf(2, cap, width),
            buf(2, count, width), buf(2, count, width), wide(2, count, width),
            buf(count, width), buf(count, width), wide(count, 128), wide(count, 128),
            pltpu.SemaphoreType.DMA((4,)), pltpu.SemaphoreType.DMA((copies,)), pltpu.SemaphoreType.DMA((copies,)),
        ],
        name="fused_layer",
        compiler_params=pltpu.CompilerParams(
            collective_id=0, has_side_effects=True, vmem_limit_bytes=56 * 1024 * 1024
        ),
    )(
        tokens, gain[None, :], w_res_in, w_res_out, w_exp_in, w_exp_out,
        expert_of[None, :], slot_of[None, :], gate_prob[None, :],
    )


def pick(mesh):
    if mesh.shape["mp"] == 4 and mesh.shape["expert"] == 4:
        return fused
    return per_device


def solution(mesh):
    return jax.shard_map(
        pick(mesh),
        mesh=mesh,
        in_specs=(
            P(("groups", "expert"), "mp"),
            P(),
            P(None, "mp"),
            P("mp", None),
            P("expert", None, "mp"),
            P("expert", "mp", None),
            P(("groups", "expert")),
            P(("groups", "expert")),
            P(("groups", "expert")),
        ),
        out_specs=P(("groups", "expert"), "mp"),
        check_vma=False,
    )
```
